32 devices in a mesh: rep: 8 (over y, x, core), ep: 4 (over z).
Axes of the slice: x: 2, y: 2, z: 4, core: 2. Of those that a mesh axis runs over, the one named last changes fastest.
Arguments:
- tokens: bfloat16 [2, 512, 4096], P(None, 'ep', 'rep'), may hold values from -6 to 6
- expert_ids: int32 [2, 512, 2], P(None, 'ep'), may hold values from 0 to 3, all different within a row; in each aligned block of 128 rows (0 to 127, 128 to 255, ..., all dimensions but the last counted through in order) at most 96 rows name the same one
- router_weight: bfloat16 [4096, 4], P('rep'), may hold values from -0.09375 to 0.09375
- w_gate: bfloat16 [4, 4096, 8192], P('ep', None, 'rep'), may hold values from -0.09375 to 0.09375
- w_up: bfloat16 [4, 4096, 8192], P('ep', None, 'rep'), may hold values from -0.09375 to 0.09375
- w_down: bfloat16 [4, 8192, 4096], P('ep', 'rep'), may hold values from -0.0625 to 0.0625
- cotangent: bfloat16 [2, 512, 4096], P(None, 'ep', 'rep'), may hold values from -6 to 6
Outputs:
- mixed: bfloat16 [2, 512, 4096], P(None, 'ep', 'rep')
- token_grad: bfloat16 [2, 512, 4096], P(None, 'ep', 'rep')
- gate_grad: bfloat16 [4, 4096, 8192], P('ep', None, 'rep')
- up_grad: bfloat16 [4, 4096, 8192], P('ep', None, 'rep')
- down_grad: bfloat16 [4, 8192, 4096], P('ep', 'rep')
- router_grad: float32 [4096, 4], P('rep')
The draws below stay inside these ranges and needn't reach their ends.
Inputs may be any that keep to these rules, and one draw needn't show every extreme that they name: `expert_ids`: each row names 2 different experts. Among the 128 rows of one index of ep in one microbatch no expert is named by more than 96 rows, and in every draw some expert is named by exactly 96 of them.
All inputs are finite; a program needn't handle non-finite values.
Results may differ from the reference program's by a relative error of at most 0.025.
Values may be sent and summed in bfloat16 or wider, within the bound.
No kernel may reach another device: no remote copies, remote signals or barrier semaphores. Data moves between devices by JAX's collectives and lax.ppermute only.
A program may use at most 192 MiB of HBM per device.

```python
import math
import jax
import jax.numpy as jnp
import numpy as np
from jax import lax

D = 4096
FF = 8192
EXPERTS = 4
TOP = 2
TOK_DEV = 128
MICRO = 2
CAP = 96
TOKENS = 512
N_REP = 8
N_EP = 4


def shard_levels(own_key, shape, shards, low, largest):
    factor_of, own = 1.0, jax.random.fold_in(own_key, 6)
    for axis_at, blocks in shards:
        draws = jnp.exp(jax.random.uniform(jax.random.fold_in(own, axis_at), (blocks,), jnp.float32, low / len(shards), largest / len(shards)))
        factor_of = factor_of * jnp.repeat(draws, shape[axis_at] // blocks).reshape([-1 if axis == axis_at else 1 for axis in range(len(shape))])
    return factor_of


def shared_out(rng, own, number, rows, number_of, top, reach, skew):
    sequence = jax.random.permutation(rng, number_of)
    packed, ordinary = shares(number_of, rows * top, reach, skew, True), shares(number_of, rows * top, reach, skew, False)
    places = jnp.arange(number_of)

    def named(tallies, turn):
        used = int((tallies > 0).sum())
        fixed = max(1, used // 4)
        passed = fixed + (places - fixed + turn * (used - fixed)) % max(1, number_of - fixed)
        return jnp.zeros((number_of,), jnp.int32).at[sequence[jnp.where(places < fixed, places, passed)]].set(jnp.asarray(tallies, jnp.int32))

    tallies = jnp.where(number % 4 == 0, named(packed, number // 4), named(ordinary, number - number // 4 - 1))
    mixed = jax.random.permutation(jax.random.fold_in(own, 3), number_of)
    donor, sink = mixed[0:number_of // 2 * 2:2], mixed[1:number_of // 2 * 2:2]
    room = jnp.minimum(tallies[donor] - 1, reach - tallies[sink]) // 2
    room = jnp.where((donor == sequence[0]) | (sink == sequence[0]) | (tallies[sink] == 0), 0, jnp.maximum(room, 0))
    passed = jax.random.randint(jax.random.fold_in(own, 4), (number_of // 2,), 0, 1 << 20) % (room + 1)
    tallies = tallies.at[donor].add(-passed).at[sink].add(passed)
    members = jnp.searchsorted(jnp.cumsum(tallies), jnp.arange(rows * top), side="right").astype(jnp.int32)
    listing = members.reshape(top, rows).T
    listing = listing[jax.random.permutation(jax.random.fold_in(own, 1), rows)]
    turn = jax.random.randint(jax.random.fold_in(own, 2), (rows, 1), 0, top)
    return jnp.take_along_axis(listing, (jnp.arange(top)[None, :] + turn) % top, axis=1)


def shares(number_of, total, reach, skew, full):
    weights = [(1 << 20) // math.isqrt(standing ** skew) + 1 for standing in range(1, number_of + 1)]
    largest = reach if full else min(reach, max(-(-total // number_of), total * weights[0] // sum(weights)))
    least = 1 if total - largest >= number_of - 1 else 0
    holding, rest = [largest] + [least] * (number_of - 1), total - largest - least * (number_of - 1)
    while rest > 0:
        candidates = [i for i in range(1, number_of) if holding[i] < largest] or [i for i in range(1, number_of) if holding[i] < reach]
        whole, budget = sum([weights[i] for i in candidates]), rest
        for i in candidates:
            addition = min(reach - holding[i], max(1, budget * weights[i] // whole), rest)
            holding[i] = holding[i] + addition
            rest = rest - addition
    return np.array(holding)


def normal_values(rng, dims, scale, bound, shards=(), kind=jnp.bfloat16):
    entries = jax.random.normal(rng, dims, jnp.float32) * scale
    if len(shards) > 0:
        entries = shard_levels(rng, dims, shards, -0.22, 0.18) * entries
    return jnp.clip(entries, min=-bound, max=bound).astype(kind)


def setup_inputs(seed: int = 0) -> dict:
    splits = jax.random.split(jax.random.key(seed), 8)
    tokens = normal_values(splits[0], (MICRO, TOKENS, D), 1.0, 6.0, ((1, 4), (2, 8)))
    expert_ids_keys = jax.random.split(jax.random.fold_in(splits[1], 1), MICRO * TOKENS // TOK_DEV)
    expert_ids_turns = jax.random.permutation(jax.random.fold_in(splits[1], 3), MICRO * TOKENS // TOK_DEV)
    expert_ids = jax.vmap(lambda own, number: shared_out(jax.random.fold_in(splits[1], 2), own, number, TOK_DEV, EXPERTS, TOP, CAP, 2))(expert_ids_keys, expert_ids_turns).reshape((MICRO, TOKENS, TOP))
    router_weight = normal_values(splits[2], (D, EXPERTS), D ** -0.5, 0.09375, ((0, 8),))
    w_gate = normal_values(splits[3], (EXPERTS, D, FF), D ** -0.5, 0.09375, ((0, 4), (2, 8)))
    w_up = normal_values(splits[4], (EXPERTS, D, FF), D ** -0.5, 0.09375, ((0, 4), (2, 8)))
    w_down = normal_values(splits[5], (EXPERTS, FF, D), FF ** -0.5, 0.0625, ((0, 4), (1, 8)))
    cotangent = normal_values(splits[6], (MICRO, TOKENS, D), 1.0, 6.0, ((1, 4), (2, 8)))
    return dict(tokens=tokens, expert_ids=expert_ids, router_weight=router_weight, w_gate=w_gate, w_up=w_up, w_down=w_down, cotangent=cotangent)


def positions(route_ids):
    hits = route_ids[:, :, None] == jnp.arange(EXPERTS, dtype=jnp.int32)[None, None, :]
    per_token = jnp.sum(hits.astype(jnp.int32), axis=1)
    before = jnp.cumsum(per_token, axis=0) - per_token
    return jnp.sum(jnp.where(hits, before[:, None, :], 0), axis=2).astype(jnp.int32)


def widen(value):
    return lax.optimization_barrier(value.astype(jnp.bfloat16)).astype(jnp.float32)


def expert_forward(rows_in, gate_w, up_w):
    pre_gate = jnp.dot(rows_in, gate_w, preferred_element_type=jnp.float32)
    pre_up = jnp.dot(rows_in, up_w, preferred_element_type=jnp.float32)
    hidden = (jax.nn.silu(pre_gate) * pre_up).astype(jnp.bfloat16)
    return pre_gate, pre_up, hidden


def grouped_down(hidden, down_w):
    group = FF // N_REP
    slots = hidden.shape[0]
    parts_h = hidden.reshape(slots, N_REP, group).transpose(1, 0, 2)
    parts_w = down_w.reshape(N_REP, group, D)

    def add(total, pair):
        return total + widen(jnp.dot(pair[0], pair[1], preferred_element_type=jnp.float32)), None

    total, _ = lax.scan(add, jnp.zeros((slots, D), jnp.float32), (parts_h, parts_w))
    return total.astype(jnp.bfloat16)


def grouped_in(gate_part, up_part, gate_w, up_w):
    group = FF // N_REP
    slots = gate_part.shape[0]
    parts_g = gate_part.reshape(slots, N_REP, group).transpose(1, 0, 2)
    parts_u = up_part.reshape(slots, N_REP, group).transpose(1, 0, 2)
    weights_g = gate_w.reshape(D, N_REP, group).transpose(1, 0, 2)
    weights_u = up_w.reshape(D, N_REP, group).transpose(1, 0, 2)

    def add(total, items):
        term = jnp.dot(items[0], items[2].T, preferred_element_type=jnp.float32)
        term = term + jnp.dot(items[1], items[3].T, preferred_element_type=jnp.float32)
        return total + widen(term), None

    total, _ = lax.scan(add, jnp.zeros((slots, D), jnp.float32), (parts_g, parts_u, weights_g, weights_u))
    return total.astype(jnp.bfloat16)


def reference(tokens, expert_ids, router_weight, w_gate, w_up, w_down, cotangent):
    slot_count = N_EP * CAP
    source = jnp.arange(TOKENS, dtype=jnp.int32) // TOK_DEV
    plans = []
    inputs = []
    for step in range(MICRO):
        route_ids = expert_ids[step].astype(jnp.int32)
        places = jax.vmap(positions)(route_ids.reshape(N_EP, TOK_DEV, TOP)).reshape(TOKENS, TOP)
        row_ids = (source[:, None] * CAP + places).astype(jnp.int32)
        values = jnp.broadcast_to(tokens[step][:, None, :], (TOKENS, TOP, D))
        inputs.append(jnp.zeros((EXPERTS, slot_count, D), jnp.bfloat16).at[route_ids, row_ids].set(values))
        plans.append((route_ids, row_ids))
    expert_in = jnp.stack(inputs, axis=1)

    def forward_one(items):
        rows_all, gate_w, up_w, down_w = items
        outs = []
        for step in range(MICRO):
            pre_gate, pre_up, hidden = expert_forward(rows_all[step], gate_w, up_w)
            outs.append(grouped_down(hidden, down_w))
        return jnp.stack(outs)

    expert_out = lax.map(forward_one, (expert_in, w_gate, w_up, w_down))
    mixed = []
    cots = []
    logit_grads = []
    router_grad = jnp.zeros((D, EXPERTS), jnp.float32)
    for step in range(MICRO):
        route_ids, row_ids = plans[step]
        logits = jnp.dot(tokens[step], router_weight, preferred_element_type=jnp.float32)
        hits = route_ids[:, :, None] == jnp.arange(EXPERTS, dtype=jnp.int32)[None, None, :]
        chosen = jnp.sum(jnp.where(hits, logits[:, None, :], 0.0), axis=2)
        spread = chosen[:, 0] - chosen[:, 1]
        gates = jnp.stack([jax.nn.sigmoid(spread), jax.nn.sigmoid(-spread)], axis=1)
        pairs = expert_out[:, step][route_ids, row_ids].astype(jnp.float32)
        mixed.append((gates[:, 0, None] * pairs[:, 0] + gates[:, 1, None] * pairs[:, 1]).astype(jnp.bfloat16))
        cot = cotangent[step].astype(jnp.float32)
        gate_dots = jnp.sum(cot[:, None, :] * pairs, axis=2)
        delta = (gate_dots[:, 0] - gate_dots[:, 1]) * gates[:, 0] * gates[:, 1]
        logit_grad = delta[:, None] * (hits[:, 0].astype(jnp.float32) - hits[:, 1].astype(jnp.float32))
        logit_grads.append(logit_grad)
        router_grad = router_grad + jnp.dot(tokens[step].astype(jnp.float32).T, logit_grad, precision=lax.Precision.HIGHEST)
        cot_pairs = (gates[:, :, None] * cot[:, None, :]).astype(jnp.bfloat16)
        cots.append(jnp.zeros((EXPERTS, slot_count, D), jnp.bfloat16).at[route_ids, row_ids].set(cot_pairs))
    expert_cot = jnp.stack(cots, axis=1)

    def backward_one(items):
        rows_all, cots_all, gate_w, up_w, down_w = items
        gate_acc = jnp.zeros((D, FF), jnp.float32)
        up_acc = jnp.zeros((D, FF), jnp.float32)
        down_acc = jnp.zeros((FF, D), jnp.float32)
        grads_in = []
        for step in range(MICRO):
            rows_in = rows_all[step]
            cot_rows = cots_all[step]
            pre_gate, pre_up, hidden = expert_forward(rows_in, gate_w, up_w)
            hidden_grad = jnp.dot(cot_rows, down_w.T, preferred_element_type=jnp.float32)
            gate_sig = jax.nn.sigmoid(pre_gate)
            gate_act = pre_gate * gate_sig
            pre_gate_grad = (hidden_grad * pre_up * (gate_sig * (1.0 + pre_gate * (1.0 - gate_sig)))).astype(jnp.bfloat16)
            pre_up_grad = (hidden_grad * gate_act).astype(jnp.bfloat16)
            down_acc = down_acc + jnp.dot(hidden.T, cot_rows, preferred_element_type=jnp.float32)
            gate_acc = gate_acc + jnp.dot(rows_in.T, pre_gate_grad, preferred_element_type=jnp.float32)
            up_acc = up_acc + jnp.dot(rows_in.T, pre_up_grad, preferred_element_type=jnp.float32)
            grads_in.append(grouped_in(pre_gate_grad, pre_up_grad, gate_w, up_w))
        return gate_acc.astype(jnp.bfloat16), up_acc.astype(jnp.bfloat16), down_acc.astype(jnp.bfloat16), jnp.stack(grads_in)

    gate_grad, up_grad, down_grad, expert_in_grad = lax.map(backward_one, (expert_in, expert_cot, w_gate, w_up, w_down))
    token_grad = []
    for step in range(MICRO):
        route_ids, row_ids = plans[step]
        pairs = expert_in_grad[:, step][route_ids, row_ids].astype(jnp.float32)
        router_in = jnp.dot(logit_grads[step], router_weight.astype(jnp.float32).T, precision=lax.Precision.HIGHEST)
        token_grad.append((pairs[:, 0] + pairs[:, 1] + router_in).astype(jnp.bfloat16))
    return jnp.stack(mixed), jnp.stack(token_grad), gate_grad, up_grad, down_grad, router_grad
```

```python
import functools

import jax
import jax.numpy as jnp
from jax import lax
from jax.experimental import pallas as pl
from jax.experimental.pallas import tpu as pltpu
from jax.sharding import PartitionSpec as P


TOP = 2
BF = jnp.bfloat16
F32 = jnp.float32
HI = lax.Precision.HIGHEST
ANY = pl.BlockSpec(memory_space=pl.ANY)


def mm(a, b):
    return jnp.dot(a, b, preferred_element_type=F32)


def mm_nt(a, b, precision=None):
    return lax.dot_general(
        a, b, (((1,), (1,)), ((), ())), preferred_element_type=F32, precision=precision
    )


def mm_tn(a, b, precision=None):
    return lax.dot_general(
        a, b, (((0,), (0,)), ((), ())), preferred_element_type=F32, precision=precision
    )


def call(kernel, grid, scalars, ins, outs, scratch=(), alias=None, flops=0, vmem=48):
    return pallas(kernel, grid, scalars, ins, outs, scratch, alias, flops, vmem)


def pallas(kernel, grid, scalars, ins, outs, scratch, alias, flops, vmem):
    return pl.pallas_call(
        kernel,
        grid_spec=pltpu.PrefetchScalarGridSpec(
            num_scalar_prefetch=len(scalars),
            grid=grid,
            in_specs=[spec for _, spec in ins],
            out_specs=[spec for _, spec in outs],
            scratch_shapes=list(scratch),
        ),
        out_shape=[shape for shape, _ in outs],
        input_output_aliases=alias or {},
        compiler_params=pltpu.CompilerParams(vmem_limit_bytes=vmem << 20),
        cost_estimate=pl.CostEstimate(flops=flops, bytes_accessed=flops // 1000, transcendentals=0),
    )(*scalars, *[array for array, _ in ins])


def whole(array):
    rank = len(array.shape)
    return pl.BlockSpec(array.shape, lambda *_: (0,) * rank)


def shape(dims, kind):
    return jax.ShapeDtypeStruct(dims, kind)


def rows_iota(rows, cols):
    return lax.broadcasted_iota(jnp.int32, (rows, cols), 0)


def slots_of(ids, step, experts, capacity, tok_rows):
    first = ids[TOP * step : TOP * step + 1, :]
    second = ids[TOP * step + 1 : TOP * step + 2, :]
    numbers = rows_iota(max(8, experts), tok_rows)
    hit_first = numbers == first
    hit_second = numbers == second
    named = (hit_first | hit_second).astype(F32)
    earlier = rows_iota(tok_rows, tok_rows) < lax.broadcasted_iota(
        jnp.int32, (tok_rows, tok_rows), 1
    )
    before = mm(named.astype(BF), earlier.astype(F32).astype(BF))
    place_first = jnp.sum(jnp.where(hit_first, before, 0.0), axis=0, keepdims=True)
    place_second = jnp.sum(jnp.where(hit_second, before, 0.0), axis=0, keepdims=True)
    return (
        first * capacity + place_first.astype(jnp.int32),
        second * capacity + place_second.astype(jnp.int32),
    )


def match(slots, step, expert, capacity, tok_rows):
    numbers = rows_iota(capacity, tok_rows) + expert * capacity
    return (
        numbers == slots[TOP * step : TOP * step + 1, :],
        numbers == slots[TOP * step + 1 : TOP * step + 2, :],
    )


def ones_of(mask):
    return mask.astype(F32).astype(BF)


def pack_tokens(me, ids, tokens, router, *outs, micro, experts, capacity):
    packed, partial, slots_out = outs[:-2], outs[-2], outs[-1]
    tok_rows = tokens.shape[1]
    listed = ids[...]
    for step in range(micro):
        first, second = slots_of(listed, step, experts, capacity, tok_rows)
        slots_out[TOP * step : TOP * step + 1, :] = first
        slots_out[TOP * step + 1 : TOP * step + 2, :] = second
        partial[experts * step : experts * (step + 1), :] = mm_nt(router[...], tokens[step])
    slots = slots_out[...]
    for turn in range(experts):
        for step in range(micro):
            a, b = match(slots, step, lax.rem(me[0] + turn, experts), capacity, tok_rows)
            packed[turn][step] = mm(ones_of(a | b), tokens[step]).astype(BF)


def pack_cots(me, ids, slots, logits, cots, *outs, micro, experts, capacity):
    packed, gates = outs[:-1], outs[-1]
    tok_rows = cots.shape[1]
    for step in range(micro):
        chosen = []
        for k in range(TOP):
            row = TOP * step + k
            named = rows_iota(experts, tok_rows) == ids[row : row + 1, :]
            part = logits[experts * step : experts * (step + 1), :]
            chosen.append(jnp.sum(jnp.where(named, part, 0.0), axis=0, keepdims=True))
        spread = chosen[0] - chosen[1]
        gates[TOP * step : TOP * step + 1, :] = jax.nn.sigmoid(spread)
        gates[TOP * step + 1 : TOP * step + 2, :] = jax.nn.sigmoid(-spread)
    listed = slots[...]
    for step in range(micro):
        for turn in range(experts):
            a, b = match(listed, step, lax.rem(me[0] + turn, experts), capacity, tok_rows)
            weight = jnp.where(a, gates[TOP * step : TOP * step + 1, :], 0.0) + jnp.where(
                b, gates[TOP * step + 1 : TOP * step + 2, :], 0.0
            )
            weight = jnp.sum(weight, axis=1, keepdims=True)
            packed[turn][step] = (mm(ones_of(a | b), cots[step]) * weight).astype(BF)


def assemble(rank, pieces, plan, out):
    slots, width = pieces[0].shape[1:]
    for piece, (step, numbers) in zip(pieces, plan):
        for i, k in enumerate(numbers):
            at = pl.multiple_of(jnp.bitwise_xor(rank, k) * width, 128)
            out[step * slots : (step + 1) * slots, pl.ds(at, width)] = piece[i]


def pre_kernel(rank, *refs, plan):
    pieces = refs[: len(plan)]
    gate_w, up_w, _, rows, hidden, pre_gate, pre_up = refs[len(plan) :]

    @pl.when(pl.program_id(0) == 0)
    def _():
        assemble(rank[0], pieces, plan, rows)

    pre_tile(rows, gate_w, up_w, hidden, pre_gate, pre_up)


def pre_rest_kernel(rows, gate_w, up_w, _a, _b, _c, _d, hidden, pre_gate, pre_up):
    pre_tile(rows, gate_w, up_w, hidden, pre_gate, pre_up)


def pre_tile(rows, gate_w, up_w, hidden, pre_gate, pre_up):
    gate = mm(rows[...], gate_w[...])
    up = mm(rows[...], up_w[...])
    pre_gate[...] = gate
    pre_up[...] = up
    hidden[...] = (gate * jax.nn.sigmoid(gate) * up).astype(BF)


def grad_kernel(rank, *refs, plan):
    pieces = refs[: len(plan)]
    down_w, hidden, pre_gate, pre_up, _, rows, gate_grad, up_grad, dots, acc = refs[len(plan) :]
    at = pl.program_id(0)

    @pl.when(at == 0)
    def _():
        assemble(rank[0], pieces, plan, rows)
        acc[...] = jnp.zeros_like(acc)

    grad = mm_nt(rows[...], down_w[...])
    gate = pre_gate[...]
    sig = jax.nn.sigmoid(gate)
    gate_grad[...] = (grad * pre_up[...] * (sig * (1.0 + gate * (1.0 - sig)))).astype(BF)
    up_grad[...] = (grad * (gate * sig)).astype(BF)
    product = grad * hidden[...].astype(F32)
    total = acc[...]
    for i in range(product.shape[1] // 128):
        total = total + product[:, 128 * i : 128 * (i + 1)]
    acc[...] = total

    @pl.when(at == pl.num_programs(0) - 1)
    def _():
        dots[...] = mm_nt(jnp.ones((8, 128), F32), acc[...], HI)


def spread(total, plan, outs):
    slots = outs[0].shape[1]
    for i, places in enumerate(plan):

        @pl.when(pl.program_id(0) == i)
        def _():
            for step, (which, at) in enumerate(places):
                outs[which][at] = total[step * slots : (step + 1) * slots, :]


def out_send_kernel(rank, hidden, down_w, _, out):
    out[...] = mm(hidden[...], down_w[...]).astype(BF)


def out_keep_kernel(rank, hidden, down_w, recv, _, *outs, plan):
    total = (mm(hidden[...], down_w[...]) + recv[...].astype(F32)).astype(BF)
    spread(total, plan, outs)


def in_send_kernel(rank, gate_g, up_g, gate_w, up_w, _, out):
    out[...] = (mm_nt(gate_g[...], gate_w[...]) + mm_nt(up_g[...], up_w[...])).astype(BF)


def in_keep_kernel(rank, gate_g, up_g, gate_w, up_w, recv, _, *outs, plan):
    total = mm_nt(gate_g[...], gate_w[...]) + mm_nt(up_g[...], up_w[...])
    spread((total + recv[...].astype(F32)).astype(BF), plan, outs)


def add_kernel(kept, recv, kept_out, sent_out):
    half = kept_out.shape[0]
    for i in range(2 * half):
        out = kept_out if i < half else sent_out
        out[i % half] = (kept[i].astype(F32) + recv[i].astype(F32)).astype(BF)


def sum_kernel(*refs, micro):
    ins, outs = refs[: 2 * micro], refs[2 * micro :]
    rows = outs[0].shape[1]
    for i, out in enumerate(outs):
        for step in range(micro):
            kept = ins[2 * step][0, i * rows : (i + 1) * rows, :].astype(F32)
            recv = ins[2 * step + 1][0, i * rows : (i + 1) * rows, :].astype(F32)
            out[step] = (kept + recv).astype(BF)


def weight_kernel(left, right, _, out):
    out[0] = mm_tn(left[...], right[...]).astype(BF)


def column_of(gates, tok_rows):
    eye = (
        rows_iota(tok_rows, tok_rows) == lax.broadcasted_iota(jnp.int32, (tok_rows, tok_rows), 1)
    ).astype(F32)
    return mm_nt(eye, gates, HI)


def mix_kernel(me, slots, gates, *refs, micro, experts, capacity):
    blocks, out = refs[:-1], refs[-1]
    tok_rows = out.shape[1]
    columns = column_of(gates[...], tok_rows)
    listed = slots[...]
    for step in range(micro):
        picked = [0.0] * TOP
        for turn in range(experts):
            hot = match(listed, step, lax.rem(me[0] + turn, experts), capacity, tok_rows)
            block = blocks[turn][step]
            for k in range(TOP):
                picked[k] = picked[k] + mm_tn(ones_of(hot[k]), block)
        total = 0.0
        for k in range(TOP):
            total = total + columns[:, TOP * step + k : TOP * step + k + 1] * picked[k]
        out[step] = total.astype(BF)


def logit_kernel(me, ids, slots, gates, tokens, dots, logit_grad, router, *, micro, experts, capacity):
    tok_rows = tokens.shape[1]
    listed = slots[...]
    total = 0.0
    for step in range(micro):
        scaled = [0.0] * TOP
        for turn in range(experts):
            hot = match(listed, step, lax.rem(me[0] + turn, experts), capacity, tok_rows)
            for k in range(TOP):
                scaled[k] = scaled[k] + lax.dot_general(
                    dots[turn], hot[k].astype(F32), (((1,), (0,)), ((), ())),
                    preferred_element_type=F32, precision=HI,
                )[step : step + 1, :]
        delta = (
            scaled[0] * gates[TOP * step + 1 : TOP * step + 2, :]
            - scaled[1] * gates[TOP * step : TOP * step + 1, :]
        )
        rows = logit_grad.shape[0] // micro
        numbers = rows_iota(rows, tok_rows)
        first = numbers == ids[TOP * step : TOP * step + 1, :]
        second = numbers == ids[TOP * step + 1 : TOP * step + 2, :]
        grad = jnp.where(first, delta, 0.0) - jnp.where(second, delta, 0.0)
        logit_grad[step * rows : (step + 1) * rows, :] = grad
        total = total + lax.dot_general(
            grad, tokens[step].astype(F32), (((1,), (0,)), ((), ())),
            preferred_element_type=F32, precision=HI,
        )
    router[...] = total


def unpack_kernel(me, slots, logit_grad, router, *refs, micro, experts, capacity):
    blocks, out = refs[:-1], refs[-1]
    tok_rows = out.shape[1]
    listed = slots[...]
    rows = logit_grad.shape[0] // micro
    for step in range(micro):
        total = mm_tn(
            logit_grad[step * rows : step * rows + experts, :], router[...].astype(F32), HI
        )
        for turn in range(experts):
            a, b = match(listed, step, lax.rem(me[0] + turn, experts), capacity, tok_rows)
            total = total + mm_tn(ones_of(a | b), blocks[turn][step])
        out[step] = total.astype(BF)


def layer(tokens, expert_ids, router_weight, w_gate, w_up, w_down, cotangent):
    micro, tok_rows, width = tokens.shape
    experts = router_weight.shape[1]
    ranks = lax.axis_size("rep")
    places = lax.axis_size("ep")
    assert places == experts and ranks & (ranks - 1) == 0 and ranks > 2
    half = ranks // 2
    capacity = min(tok_rows, 3 * tok_rows * TOP // (2 * experts))
    slots_n = places * capacity
    gate_w, up_w, down_w = w_gate[0], w_up[0], w_down[0]
    features, units = gate_w.shape
    rank = lax.axis_index("rep").reshape(1)
    me = lax.axis_index("ep").reshape(1)
    sizes = dict(micro=micro, experts=experts, capacity=capacity)

    def swap(value, bits):
        return lax.ppermute(value, "rep", [(i, i ^ bits) for i in range(ranks)])

    def shift(value, turn):
        return lax.ppermute(value, "ep", [(i, (i + turn) % places) for i in range(places)])

    def full(array):
        return (array, whole(array))

    ids = jnp.transpose(expert_ids, (0, 2, 1)).reshape(micro * TOP, tok_rows)
    router = router_weight.T

    block = shape((micro, capacity, width), BF)
    token_rows = shape((micro * TOP, tok_rows), jnp.int32)
    logit_rows = shape((micro * experts, tok_rows), F32)
    *packed, logits, slots = call(
        functools.partial(pack_tokens, **sizes), (1,), [me],
        [full(ids), full(tokens), full(router)],
        [full(block)] * experts + [full(logit_rows), full(token_rows)],
        flops=10**8,
    )
    bits = 1
    while bits < ranks:
        logits = logits + swap(logits, bits)
        bits *= 2
    *cots, gates = call(
        functools.partial(pack_cots, **sizes), (1,), [me],
        [full(ids), full(slots), full(logits), full(cotangent)],
        [full(block)] * experts + [full(shape((micro * TOP, tok_rows), F32))],
        flops=10**8,
    )
    chip_bits = [1 << i for i in range(1, ranks.bit_length() - 1)]
    order = [chip_bits[m % len(chip_bits) :] + chip_bits[: m % len(chip_bits)] for m in range(micro)]

    def deliver(blocks):
        got = [blocks[0]] + [shift(blocks[turn], turn) for turn in range(1, places)]
        pieces, plan = [], []
        held, numbers = [], []
        for step in range(micro):
            held.append(jnp.concatenate([part[step : step + 1] for part in got], axis=1))
            numbers.append([0])
        for stage in range(len(chip_bits)):
            for step in range(micro):
                bit = order[step][stage]
                recv = swap(held[step], bit)
                there = [k ^ bit for k in numbers[step]]
                if stage == len(chip_bits) - 1:
                    pieces += [held[step], recv]
                    plan += [(step, numbers[step]), (step, there)]
                else:
                    held[step] = jnp.concatenate([held[step], recv], axis=0)
                    numbers[step] = numbers[step] + there
        for i in range(len(pieces)):
            pieces.append(swap(pieces[i], 1))
            plan.append((plan[i][0], [k ^ 1 for k in plan[i][1]]))
        return pieces, plan

    token_pieces, plan = deliver(packed)
    cot_pieces, _ = deliver(cots)

    tile = min(256, units // 2)
    steps = units // tile
    part = steps // 2
    all_rows = micro * slots_n
    work = 2 * all_rows * features * units
    columns = pl.BlockSpec((all_rows, tile), lambda i, *_: (0, i))
    rows_shape = shape((all_rows, features), BF)
    units_shape = shape((all_rows, units), BF)
    wide_shape = shape((all_rows, units), F32)

    weight = pl.BlockSpec((features, tile), lambda i, *_: (0, i))
    rows_in, *firsts = call(
        functools.partial(pre_kernel, plan=plan), (part,), [rank],
        [full(p) for p in token_pieces] + [(gate_w, weight), (up_w, weight), (cots[0], ANY)],
        [full(rows_shape), (units_shape, columns)] + [(wide_shape, columns)] * 2,
        flops=work,
    )
    weight = pl.BlockSpec((features, tile), lambda i: (0, i + part))
    later = pl.BlockSpec((all_rows, tile), lambda i: (0, i + part))
    hidden, pre_gate, pre_up = call(
        pre_rest_kernel, (part,), [],
        [full(rows_in), (gate_w, weight), (up_w, weight)]
        + [(array, ANY) for array in firsts] + [(gates, ANY)],
        [(units_shape, later)] + [(wide_shape, later)] * 2,
        alias={3: 0, 4: 1, 5: 2},
        flops=work,
    )
    sent = shape((half, all_rows, width), BF)
    kept = shape((half // 2, slots_n, width), BF)
    by_step = pl.BlockSpec((None, all_rows, width), lambda i, *_: (i, 0, 0))
    lists = []
    for step in range(micro):
        numbers = [0]
        for bit in order[step]:
            numbers = numbers + [k ^ bit for k in numbers]
        lists.append(numbers)
    homes = []
    for i in range(half):
        at = [lists[step].index(2 * i) for step in range(micro)]
        homes.append(
            [(2 * step + at[step] // (half // 2), at[step] % (half // 2)) for step in range(micro)]
        )

    def wide(odd):
        return pl.BlockSpec((units, width), lambda i, r: (0, jnp.bitwise_xor(r[0], 2 * i + odd)))

    def tall(odd):
        return pl.BlockSpec((width, units), lambda i, r: (jnp.bitwise_xor(r[0], 2 * i + odd), 0))

    def reduce(parts):
        parts = list(parts)
        for stage in reversed(range(len(chip_bits))):
            for step in range(micro):
                mine, theirs = parts[2 * step], parts[2 * step + 1]
                recv = swap(theirs, order[step][stage])
                if stage == 0:
                    parts[2 * step + 1] = recv
                else:
                    smaller = shape((mine.shape[0] // 2,) + mine.shape[1:], BF)
                    parts[2 * step], parts[2 * step + 1] = call(
                        add_kernel, (1,), [], [full(mine), full(recv)], [full(smaller)] * 2, flops=10**7
                    )
        blocks = call(
            functools.partial(sum_kernel, micro=micro), (1,), [],
            [full(part) for part in parts], [full(block)] * places, flops=10**7,
        )
        return [blocks[0]] + [shift(blocks[turn], -turn) for turn in range(1, places)]

    (out_sent,) = call(
        out_send_kernel, (half,), [rank],
        [full(hidden), (down_w, wide(1)), (hidden, ANY)], [(sent, by_step)], flops=work // 2,
    )
    out_parts = call(
        functools.partial(out_keep_kernel, plan=homes), (half,), [rank],
        [full(hidden), (down_w, wide(0)), (swap(out_sent, 1), by_step), (hidden, ANY)],
        [full(kept)] * (2 * micro), flops=work // 2,
    )
    out_blocks = reduce(out_parts)

    weight = pl.BlockSpec((tile, features), lambda i, *_: (i, 0))
    rows_cot, gate_g, up_g, dots = call(
        functools.partial(grad_kernel, plan=plan), (steps,), [rank],
        [full(p) for p in cot_pieces]
        + [(down_w, weight), (hidden, columns), (pre_gate, columns), (pre_up, columns)]
        + [(out_parts[0], ANY)],
        [full(rows_shape), (units_shape, columns), (units_shape, columns)]
        + [full(shape((8, all_rows), F32))],
        scratch=[pltpu.VMEM((all_rows, 128), F32)],
        flops=work,
    )
    (in_sent,) = call(
        in_send_kernel, (half,), [rank],
        [full(gate_g), full(up_g), (gate_w, tall(1)), (up_w, tall(1)), (dots, ANY)],
        [(sent, by_step)], flops=work,
    )
    in_parts = call(
        functools.partial(in_keep_kernel, plan=homes), (half,), [rank],
        [full(gate_g), full(up_g), (gate_w, tall(0)), (up_w, tall(0))]
        + [(swap(in_sent, 1), by_step), (in_sent, ANY)],
        [full(kept)] * (2 * micro), flops=work,
    )
    in_blocks = reduce(in_parts)
    span = min(512, features)
    rows_span = pl.BlockSpec((all_rows, span), lambda i: (0, i))
    down_spec = pl.BlockSpec((1, units, span), lambda i: (0, 0, i))
    (down_grad,) = call(
        weight_kernel, (features // span,), [],
        [full(hidden), (rows_cot, rows_span), (in_parts[0], ANY)],
        [(shape((1, units, features), BF), down_spec)],
        flops=work,
    )
    last, grads = down_grad, []
    for g in (gate_g, up_g):
        (last,) = call(
            weight_kernel, (features // span,), [],
            [(rows_in, rows_span), full(g), (last, ANY)],
            [(shape((1, features, units), BF), pl.BlockSpec((1, span, units), lambda i: (0, i, 0)))],
            flops=work,
        )
        grads.append(last)
    gate_grad, up_grad = grads

    scaled = dots[0].reshape(micro, places, capacity)
    scaled = jnp.pad(scaled, ((0, 8 - micro), (0, 0), (0, 0)))
    home = jnp.stack([scaled[:, 0]] + [shift(scaled[:, turn], -turn) for turn in range(1, places)])
    bits = 1
    while bits < ranks:
        home = home + swap(home, bits)
        bits *= 2
    (mixed,) = call(
        functools.partial(mix_kernel, **sizes), (1,), [me],
        [full(slots), full(gates)] + [full(b) for b in out_blocks],
        [full(shape(tokens.shape, BF))], flops=10**8,
    )
    padded = max(8, experts)
    logit_grad, router_grad = call(
        functools.partial(logit_kernel, **sizes), (1,), [me],
        [full(ids), full(slots), full(gates), full(tokens), full(home)],
        [full(shape((micro * padded, tok_rows), F32)), full(shape((padded, width), F32))],
        flops=10**8,
    )
    bits = 1
    while bits < places:
        theirs = lax.ppermute(router_grad, "ep", [(i, i ^ bits) for i in range(places)])
        router_grad = router_grad + theirs
        bits *= 2
    (token_grad,) = call(
        functools.partial(unpack_kernel, **sizes), (1,), [me],
        [full(slots), full(logit_grad), full(router)] + [full(b) for b in in_blocks],
        [full(shape(tokens.shape, BF))], flops=10**8,
    )
    return mixed, token_grad, gate_grad, up_grad, down_grad, router_grad[:experts].T


def solution(mesh):
    in_specs = (
        P(None, "ep", "rep"),
        P(None, "ep", None),
        P("rep", None),
        P("ep", None, "rep"),
        P("ep", None, "rep"),
        P("ep", "rep", None),
        P(None, "ep", "rep"),
    )
    out_specs = (
        P(None, "ep", "rep"),
        P(None, "ep", "rep"),
        P("ep", None, "rep"),
        P("ep", None, "rep"),
        P("ep", "rep", None),
        P("rep", None),
    )
    return jax.shard_map(layer, mesh=mesh, in_specs=in_specs, out_specs=out_specs, check_vma=False)
```

```python
import contextlib
import functools

import jax
import jax.numpy as jnp
from jax import lax
from jax.experimental import pallas as pl
from jax.experimental.pallas import tpu as pltpu
from jax.sharding import PartitionSpec as P


TOP = 2
BF = jnp.bfloat16
F32 = jnp.float32
HI = lax.Precision.HIGHEST
ANY = pl.BlockSpec(memory_space=pl.ANY)


def mm(a, b):
    return jnp.dot(a, b, preferred_element_type=F32)


def mm_nt(a, b, precision=None):
    return lax.dot_general(
        a, b, (((1,), (1,)), ((), ())), preferred_element_type=F32, precision=precision
    )


def mm_tn(a, b, precision=None):
    return lax.dot_general(
        a, b, (((0,), (0,)), ((), ())), preferred_element_type=F32, precision=precision
    )


def call(kernel, grid, scalars, ins, outs, scratch=(), alias=None, flops=0, vmem=20):
    return pallas(kernel, grid, scalars, ins, outs, scratch, alias, flops, vmem)


def pallas(kernel, grid, scalars, ins, outs, scratch, alias, flops, vmem):
    return pl.pallas_call(
        kernel,
        grid_spec=pltpu.PrefetchScalarGridSpec(
            num_scalar_prefetch=len(scalars),
            grid=grid,
            in_specs=[spec for _, spec in ins],
            out_specs=[spec for _, spec in outs],
            scratch_shapes=list(scratch),
        ),
        out_shape=[shape for shape, _ in outs],
        input_output_aliases=alias or {},
        compiler_params=pltpu.CompilerParams(vmem_limit_bytes=vmem << 20),
        cost_estimate=pl.CostEstimate(flops=flops, bytes_accessed=flops // 1000, transcendentals=0),
    )(*scalars, *[array for array, _ in ins])


def whole(array):
    rank = len(array.shape)
    return pl.BlockSpec(array.shape, lambda *_: (0,) * rank)


def shape(dims, kind):
    return jax.ShapeDtypeStruct(dims, kind)


def rows_iota(rows, cols):
    return lax.broadcasted_iota(jnp.int32, (rows, cols), 0)


def slots_of(ids, step, experts, capacity, tok_rows):
    first = ids[TOP * step : TOP * step + 1, :]
    second = ids[TOP * step + 1 : TOP * step + 2, :]
    numbers = rows_iota(max(8, experts), tok_rows)
    hit_first = numbers == first
    hit_second = numbers == second
    named = (hit_first | hit_second).astype(F32)
    earlier = rows_iota(tok_rows, tok_rows) < lax.broadcasted_iota(
        jnp.int32, (tok_rows, tok_rows), 1
    )
    before = mm(named.astype(BF), earlier.astype(F32).astype(BF))
    place_first = jnp.sum(jnp.where(hit_first, before, 0.0), axis=0, keepdims=True)
    place_second = jnp.sum(jnp.where(hit_second, before, 0.0), axis=0, keepdims=True)
    return (
        first * capacity + place_first.astype(jnp.int32),
        second * capacity + place_second.astype(jnp.int32),
    )


def match(slots, step, expert, capacity, tok_rows):
    numbers = rows_iota(capacity, tok_rows) + expert * capacity
    return (
        numbers == slots[TOP * step : TOP * step + 1, :],
        numbers == slots[TOP * step + 1 : TOP * step + 2, :],
    )


def ones_of(mask):
    return mask.astype(F32).astype(BF)


def pack_tokens(me, ids, tokens, router, *outs, micro, experts, capacity):
    packed, partial, slots_out = outs[:-2], outs[-2], outs[-1]
    tok_rows = tokens.shape[1]
    listed = ids[...]
    for step in range(micro):
        first, second = slots_of(listed, step, experts, capacity, tok_rows)
        slots_out[TOP * step : TOP * step + 1, :] = first
        slots_out[TOP * step + 1 : TOP * step + 2, :] = second
        partial[experts * step : experts * (step + 1), :] = mm_nt(router[...], tokens[step])
    slots = slots_out[...]
    for turn in range(experts):
        for step in range(micro):
            a, b = match(slots, step, lax.rem(me[0] + turn, experts), capacity, tok_rows)
            packed[turn][step] = mm(ones_of(a | b), tokens[step]).astype(BF)


def pack_cots(me, ids, slots, logits, cots, *outs, micro, experts, capacity):
    packed, gates = outs[:-1], outs[-1]
    tok_rows = cots.shape[1]
    for step in range(micro):
        chosen = []
        for k in range(TOP):
            row = TOP * step + k
            named = rows_iota(experts, tok_rows) == ids[row : row + 1, :]
            part = logits[experts * step : experts * (step + 1), :]
            chosen.append(jnp.sum(jnp.where(named, part, 0.0), axis=0, keepdims=True))
        spread = chosen[0] - chosen[1]
        gates[TOP * step : TOP * step + 1, :] = jax.nn.sigmoid(spread)
        gates[TOP * step + 1 : TOP * step + 2, :] = jax.nn.sigmoid(-spread)
    listed = slots[...]
    for step in range(micro):
        for turn in range(experts):
            a, b = match(listed, step, lax.rem(me[0] + turn, experts), capacity, tok_rows)
            weight = jnp.where(a, gates[TOP * step : TOP * step + 1, :], 0.0) + jnp.where(
                b, gates[TOP * step + 1 : TOP * step + 2, :], 0.0
            )
            weight = jnp.sum(weight, axis=1, keepdims=True)
            packed[turn][step] = (mm(ones_of(a | b), cots[step]) * weight).astype(BF)


def assemble(rank, pieces, plan, out):
    slots, width = pieces[0].shape[1:]
    for piece, entries in zip(pieces, plan):
        for i, (step, k) in enumerate(entries):
            at = pl.multiple_of(jnp.bitwise_xor(rank, k) * width, 128)
            out[step * slots : (step + 1) * slots, pl.ds(at, width)] = piece[i]


@contextlib.contextmanager
def keep_rows(rank, pieces, plan, rows, rows_out, sem):
    copy = pltpu.make_async_copy(rows, rows_out, sem)

    @pl.when(pl.program_id(0) == 0)
    def _():
        assemble(rank[0], pieces, plan, rows)
        copy.start()

    yield

    @pl.when(pl.program_id(0) == pl.num_programs(0) - 1)
    def _():
        copy.wait()


def pre_kernel(rank, *refs, plan):
    pieces = refs[: len(plan)]
    gate_w, up_w, rows_out, hidden, pre_gate, pre_up, rows, sem = refs[len(plan) :]

    with keep_rows(rank, pieces, plan, rows, rows_out, sem):
        pre_tile(rows, gate_w, up_w, hidden, pre_gate, pre_up)


def pre_tile(rows, gate_w, up_w, hidden, pre_gate, pre_up):
    gate = mm(rows[...], gate_w[...])
    up = mm(rows[...], up_w[...])
    pre_gate[...] = gate
    pre_up[...] = up
    hidden[...] = (gate * jax.nn.sigmoid(gate) * up).astype(BF)


def grad_kernel(rank, *refs, plan):
    pieces = refs[: len(plan)]
    down_w, hidden, pre_gate, pre_up, _, rows_out, gate_grad, up_grad, dots, rows, acc, sem = refs[
        len(plan) :
    ]
    at = pl.program_id(0)

    @pl.when(at == 0)
    def _():
        acc[...] = jnp.zeros_like(acc)

    with keep_rows(rank, pieces, plan, rows, rows_out, sem):
        grad = mm_nt(rows[...], down_w[...])
        gate = pre_gate[...]
        sig = jax.nn.sigmoid(gate)
        gate_grad[...] = (grad * pre_up[...] * (sig * (1.0 + gate * (1.0 - sig)))).astype(BF)
        up_grad[...] = (grad * (gate * sig)).astype(BF)
        product = grad * hidden[...].astype(F32)
        total = acc[...]
        for i in range(product.shape[1] // 128):
            total = total + product[:, 128 * i : 128 * (i + 1)]
        acc[...] = total

        @pl.when(at == pl.num_programs(0) - 1)
        def _():
            dots[...] = mm_nt(jnp.ones((8, 128), F32), acc[...], HI)


def spread(total, plan, outs):
    slots = outs[0].shape[1]
    for i, places in enumerate(plan):

        @pl.when(pl.program_id(0) == i)
        def _():
            for step, (which, at) in enumerate(places):
                outs[which][at] = total[step * slots : (step + 1) * slots, :]


def out_send_kernel(rank, hidden, down_w, _, out):
    out[...] = mm(hidden[...], down_w[...]).astype(BF)


def out_keep_kernel(rank, hidden, down_w, recv, _, *outs):
    total = (mm(hidden[...], down_w[...]) + recv[...].astype(F32)).astype(BF)
    for i, out in enumerate(outs):
        pl.when(pl.program_id(0) == i)(functools.partial(out.__setitem__, Ellipsis, total))


def in_send_kernel(rank, gate_g, up_g, gate_w, up_w, _, out):
    out[...] = (mm_nt(gate_g[...], gate_w[...]) + mm_nt(up_g[...], up_w[...])).astype(BF)


def in_keep_kernel(rank, gate_g, up_g, gate_w, up_w, recv, _, *outs, plan):
    total = mm_nt(gate_g[...], gate_w[...]) + mm_nt(up_g[...], up_w[...])
    spread((total + recv[...].astype(F32)).astype(BF), plan, outs)


def add_kernel(kept, recv, kept_out, sent_out):
    half = kept_out.shape[0]
    for i in range(2 * half):
        out = kept_out if i < half else sent_out
        out[i % half] = (kept[i].astype(F32) + recv[i].astype(F32)).astype(BF)


def sum_kernel(*refs, micro):
    ins, outs = refs[: 2 * micro], refs[2 * micro :]
    rows = outs[0].shape[1]
    for i, out in enumerate(outs):
        for step in range(micro):
            kept = ins[2 * step][0, i * rows : (i + 1) * rows, :].astype(F32)
            recv = ins[2 * step + 1][0, i * rows : (i + 1) * rows, :].astype(F32)
            out[step] = (kept + recv).astype(BF)


def sum_all_kernel(*refs):
    outs = [ref for ref in refs if len(ref.shape) == 3]
    terms = refs[: len(refs) - len(outs)]
    micro, rows, _ = outs[0].shape
    for step in range(micro):
        for i, out in enumerate(outs):
            at = (step * len(outs) + i) * rows
            total = terms[0][at : at + rows, :].astype(F32)
            for term in terms[1:]:
                total = total + term[at : at + rows, :].astype(F32)
            out[step] = total.astype(BF)


def weight_in_kernel(rows, gate_g, up_g, *refs):
    gate_out, up_out = refs[-2:]
    left = rows[...]
    gate_out[0] = mm_tn(left, gate_g[...]).astype(BF)
    up_out[0] = mm_tn(left, up_g[...]).astype(BF)


def weight_down_kernel(hidden, cots, _, out):
    out[0] = mm_tn(hidden[...], cots[...]).astype(BF)


def column_of(gates, tok_rows):
    eye = (
        rows_iota(tok_rows, tok_rows) == lax.broadcasted_iota(jnp.int32, (tok_rows, tok_rows), 1)
    ).astype(F32)
    return mm_nt(eye, gates, HI)


def mix_kernel(me, slots, gates, *refs, micro, experts, capacity):
    blocks, out = refs[:-1], refs[-1]
    tok_rows = out.shape[1]
    columns = column_of(gates[...], tok_rows)
    listed = slots[...]
    for step in range(micro):
        picked = [0.0] * TOP
        for turn in range(experts):
            hot = match(listed, step, lax.rem(me[0] + turn, experts), capacity, tok_rows)
            block = blocks[turn][step]
            for k in range(TOP):
                picked[k] = picked[k] + mm_tn(ones_of(hot[k]), block)
        total = 0.0
        for k in range(TOP):
            total = total + columns[:, TOP * step + k : TOP * step + k + 1] * picked[k]
        out[step] = total.astype(BF)


def logit_kernel(me, ids, slots, gates, tokens, dots, logit_grad, router, *, micro, experts, capacity):
    tok_rows = tokens.shape[1]
    listed = slots[...]
    total = 0.0
    for step in range(micro):
        scaled = [0.0] * TOP
        for turn in range(experts):
            hot = match(listed, step, lax.rem(me[0] + turn, experts), capacity, tok_rows)
            for k in range(TOP):
                scaled[k] = scaled[k] + lax.dot_general(
                    dots[turn], hot[k].astype(F32), (((1,), (0,)), ((), ())),
                    preferred_element_type=F32, precision=HI,
                )[step : step + 1, :]
        delta = (
            scaled[0] * gates[TOP * step + 1 : TOP * step + 2, :]
            - scaled[1] * gates[TOP * step : TOP * step + 1, :]
        )
        rows = logit_grad.shape[0] // micro
        numbers = rows_iota(rows, tok_rows)
        first = numbers == ids[TOP * step : TOP * step + 1, :]
        second = numbers == ids[TOP * step + 1 : TOP * step + 2, :]
        grad = jnp.where(first, delta, 0.0) - jnp.where(second, delta, 0.0)
        logit_grad[step * rows : (step + 1) * rows, :] = grad
        total = total + lax.dot_general(
            grad, tokens[step].astype(F32), (((1,), (0,)), ((), ())),
            preferred_element_type=F32, precision=HI,
        )
    router[...] = total


def unpack_kernel(me, slots, logit_grad, router, *refs, micro, experts, capacity):
    blocks, out = refs[:-1], refs[-1]
    tok_rows = out.shape[1]
    listed = slots[...]
    rows = logit_grad.shape[0] // micro
    for step in range(micro):
        total = mm_tn(
            logit_grad[step * rows : step * rows + experts, :], router[...].astype(F32), HI
        )
        for turn in range(experts):
            a, b = match(listed, step, lax.rem(me[0] + turn, experts), capacity, tok_rows)
            total = total + mm_tn(ones_of(a | b), blocks[turn][step])
        out[step] = total.astype(BF)


def layer(tokens, expert_ids, router_weight, w_gate, w_up, w_down, cotangent):
    micro, tok_rows, width = tokens.shape
    experts = router_weight.shape[1]
    ranks = lax.axis_size("rep")
    places = lax.axis_size("ep")
    assert places == experts and ranks & (ranks - 1) == 0 and ranks > 2
    half = ranks // 2
    capacity = min(tok_rows, 3 * tok_rows * TOP // (2 * experts))
    slots_n = places * capacity
    gate_w, up_w, down_w = w_gate[0], w_up[0], w_down[0]
    features, units = gate_w.shape
    rank = lax.axis_index("rep").reshape(1)
    me = lax.axis_index("ep").reshape(1)
    sizes = dict(micro=micro, experts=experts, capacity=capacity)

    def swap(value, bits):
        return lax.ppermute(value, "rep", [(i, i ^ bits) for i in range(ranks)])

    def shift(value, turn):
        return lax.ppermute(value, "ep", [(i, (i + turn) % places) for i in range(places)])

    def far(array):
        return pltpu.with_memory_space_constraint(array, pltpu.HBM)

    def full(array):
        return (array, whole(array))

    ids = jnp.transpose(expert_ids, (0, 2, 1)).reshape(micro * TOP, tok_rows)
    router = router_weight.T

    block = shape((micro, capacity, width), BF)
    token_rows = shape((micro * TOP, tok_rows), jnp.int32)
    logit_rows = shape((micro * experts, tok_rows), F32)
    *packed, logits, slots = call(
        functools.partial(pack_tokens, **sizes), (1,), [me],
        [full(ids), full(tokens), full(router)],
        [full(block)] * experts + [full(logit_rows), full(token_rows)],
        flops=10**8,
    )
    bits = 1
    while bits < ranks:
        logits = logits + swap(logits, bits)
        bits *= 2
    *cots, gates = call(
        functools.partial(pack_cots, **sizes), (1,), [me],
        [full(ids), full(slots), full(logits), full(cotangent)],
        [full(block)] * experts + [full(shape((micro * TOP, tok_rows), F32))],
        flops=10**8,
    )
    chip_bits = [1 << i for i in range(1, ranks.bit_length() - 1)]
    order = [chip_bits[m % len(chip_bits) :] + chip_bits[: m % len(chip_bits)] for m in range(micro)]

    def dispatch(blocks):
        got = [blocks[0]]
        for turn in range(1, places):
            got.append(shift(blocks[turn], turn))
        return got

    def to_partner(pieces, plan):
        for i in range(len(pieces)):
            pieces.append(swap(pieces[i], 1))
            plan.append([(step, k ^ 1) for step, k in plan[i]])
        return pieces, plan

    def gather_by_steps(blocks):
        got = dispatch(blocks)
        pieces, plan = [], []
        held, numbers = [], []
        for step in range(micro):
            held.append(jnp.concatenate([part[step : step + 1] for part in got], axis=1))
            numbers.append([(step, 0)])
        for stage in range(len(chip_bits)):
            for step in range(micro):
                bit = order[step][stage]
                recv = swap(held[step], bit)
                there = [(step, k ^ bit) for _, k in numbers[step]]
                if stage == len(chip_bits) - 1:
                    pieces += [held[step], recv]
                    plan += [numbers[step], there]
                else:
                    held[step] = jnp.concatenate([held[step], recv], axis=0)
                    numbers[step] = numbers[step] + there
        return to_partner(pieces, plan)

    def gather_at_once(blocks):
        own = jnp.concatenate(dispatch(blocks), axis=1)
        pieces = [own] + [swap(own, 2 * k) for k in range(1, half)]
        plan = [[(step, 2 * k) for step in range(micro)] for k in range(half)]
        return to_partner(pieces, plan)

    token_pieces, token_plan = gather_by_steps(packed)
    cot_pieces, cot_plan = gather_at_once(cots)

    tile = min(256, units)
    steps = units // tile
    all_rows = micro * slots_n
    work = 2 * all_rows * features * units
    columns = pl.BlockSpec((all_rows, tile), lambda i, *_: (0, i))
    rows_shape = shape((all_rows, features), BF)
    units_shape = shape((all_rows, units), BF)
    wide_shape = shape((all_rows, units), F32)

    weight = pl.BlockSpec((features, tile), lambda i, *_: (0, i))
    rows_in, hidden, pre_gate, pre_up = call(
        functools.partial(pre_kernel, plan=token_plan), (steps,), [rank],
        [full(p) for p in token_pieces] + [(far(gate_w), weight), (far(up_w), weight)],
        [(rows_shape, ANY), (units_shape, columns)] + [(wide_shape, columns)] * 2,
        scratch=[pltpu.VMEM((all_rows, features), BF), pltpu.SemaphoreType.DMA],
        flops=2 * work,
        vmem=36,
    )
    sent = shape((half, all_rows, width), BF)
    kept = shape((half // 2, slots_n, width), BF)
    by_step = pl.BlockSpec((None, all_rows, width), lambda i, *_: (i, 0, 0))
    lists = []
    for step in range(micro):
        numbers = [0]
        for bit in order[step]:
            numbers = numbers + [k ^ bit for k in numbers]
        lists.append(numbers)
    homes = []
    for i in range(half):
        at = [lists[step].index(2 * i) for step in range(micro)]
        homes.append(
            [(2 * step + at[step] // (half // 2), at[step] % (half // 2)) for step in range(micro)]
        )

    def wide(odd):
        return pl.BlockSpec((units, width), lambda i, r: (0, jnp.bitwise_xor(r[0], 2 * i + odd)))

    def tall(odd):
        return pl.BlockSpec((width, units), lambda i, r: (jnp.bitwise_xor(r[0], 2 * i + odd), 0))

    def reduce(parts):
        parts = list(parts)
        for stage in reversed(range(len(chip_bits))):
            for step in range(micro):
                mine, theirs = parts[2 * step], parts[2 * step + 1]
                recv = swap(theirs, order[step][stage])
                if stage == 0:
                    parts[2 * step + 1] = recv
                else:
                    smaller = shape((mine.shape[0] // 2,) + mine.shape[1:], BF)
                    parts[2 * step], parts[2 * step + 1] = call(
                        add_kernel, (1,), [], [full(mine), full(recv)], [full(smaller)] * 2, flops=10**7
                    )
        blocks = call(
            functools.partial(sum_kernel, micro=micro), (1,), [],
            [full(part) for part in parts], [full(block)] * places, flops=10**7,
        )
        return send_home(blocks)

    def send_home(blocks):
        return [blocks[0]] + [shift(blocks[turn], -turn) for turn in range(1, places)]

    (out_sent,) = call(
        out_send_kernel, (half,), [rank],
        [full(hidden), (far(down_w), wide(1)), (hidden, ANY)], [(sent, by_step)], flops=work // 2,
    )
    out_parts = call(
        out_keep_kernel, (half,), [rank],
        [full(hidden), (far(down_w), wide(0)), (swap(out_sent, 1), by_step), (hidden, ANY)],
        [full(shape((all_rows, width), BF))] * half, flops=work // 2,
    )
    out_terms = [out_parts[0]] + [swap(out_parts[k], 2 * k) for k in range(1, half)]
    out_blocks = send_home(
        call(sum_all_kernel, (1,), [], [full(t) for t in out_terms], [full(block)] * places, flops=10**7)
    )

    weight = pl.BlockSpec((tile, features), lambda i, *_: (i, 0))
    rows_cot, gate_g, up_g, dots = call(
        functools.partial(grad_kernel, plan=cot_plan), (steps,), [rank],
        [full(p) for p in cot_pieces]
        + [(far(down_w), weight), (hidden, columns), (pre_gate, columns), (pre_up, columns)]
        + [(out_parts[0], ANY)],
        [(rows_shape, ANY), (units_shape, columns), (units_shape, columns)]
        + [full(shape((8, all_rows), F32))],
        scratch=[pltpu.VMEM((all_rows, features), BF), pltpu.VMEM((all_rows, 128), F32), pltpu.SemaphoreType.DMA],
        flops=work,
        vmem=36,
    )
    (in_sent,) = call(
        in_send_kernel, (half,), [rank],
        [full(gate_g), full(up_g), (far(gate_w), tall(1)), (far(up_w), tall(1)), (dots, ANY)],
        [(sent, by_step)], flops=work,
    )
    in_parts = call(
        functools.partial(in_keep_kernel, plan=homes), (half,), [rank],
        [full(gate_g), full(up_g), (far(gate_w), tall(0)), (far(up_w), tall(0))]
        + [(swap(in_sent, 1), by_step), (in_sent, ANY)],
        [full(kept)] * (2 * micro), flops=work, vmem=26,
    )
    in_blocks = reduce(in_parts)
    span = min(512, features)
    rows_span = pl.BlockSpec((all_rows, span), lambda i: (0, i))
    part = features // span // 2
    grads = [in_parts[0]]
    for base in (0, part):
        weight_spec = pl.BlockSpec((1, span, units), lambda i, base=base: (0, i + base, 0))
        rows_part = pl.BlockSpec((all_rows, span), lambda i, base=base: (0, i + base))
        grads = call(
            weight_in_kernel, (part,), [],
            [(far(rows_in), rows_part), full(gate_g), full(up_g)] + [(far(g) if base else g, ANY) for g in grads],
            [(pltpu.HBM((1, features, units), BF), weight_spec)] * 2,
            alias={3: 0, 4: 1} if base else None,
            flops=work,
        )
    gate_grad, up_grad = grads
    span = min(1024, features)
    rows_span = pl.BlockSpec((all_rows, span), lambda i: (0, i))
    down_spec = pl.BlockSpec((1, units, span), lambda i: (0, 0, i))
    (down_grad,) = call(
        weight_down_kernel, (features // span,), [],
        [full(hidden), (far(rows_cot), rows_span), (dots, ANY)],
        [(pltpu.HBM((1, units, features), BF), down_spec)],
        flops=work,
    )

    scaled = dots[0].reshape(micro, places, capacity)
    scaled = jnp.pad(scaled, ((0, 8 - micro), (0, 0), (0, 0)))
    home = jnp.stack([scaled[:, 0]] + [shift(scaled[:, turn], -turn) for turn in range(1, places)])
    bits = 1
    while bits < ranks:
        home = home + swap(home, bits)
        bits *= 2
    (mixed,) = call(
        functools.partial(mix_kernel, **sizes), (1,), [me],
        [full(slots), full(gates)] + [full(b) for b in out_blocks],
        [full(shape(tokens.shape, BF))], flops=10**8,
    )
    padded = max(8, experts)
    logit_grad, router_grad = call(
        functools.partial(logit_kernel, **sizes), (1,), [me],
        [full(ids), full(slots), full(gates), full(tokens), full(home)],
        [full(shape((micro * padded, tok_rows), F32)), full(shape((padded, width), F32))],
        flops=10**8,
    )
    bits = 1
    while bits < places:
        theirs = lax.ppermute(router_grad, "ep", [(i, i ^ bits) for i in range(places)])
        router_grad = router_grad + theirs
        bits *= 2
    (token_grad,) = call(
        functools.partial(unpack_kernel, **sizes), (1,), [me],
        [full(slots), full(logit_grad), full(router)] + [full(b) for b in in_blocks],
        [full(shape(tokens.shape, BF))], flops=10**8,
    )
    return mixed, token_grad, gate_grad, up_grad, down_grad, router_grad[:experts].T


def solution(mesh):
    in_specs = (
        P(None, "ep", "rep"),
        P(None, "ep", None),
        P("rep", None),
        P("ep", None, "rep"),
        P("ep", None, "rep"),
        P("ep", "rep", None),
        P(None, "ep", "rep"),
    )
    out_specs = (
        P(None, "ep", "rep"),
        P(None, "ep", "rep"),
        P("ep", None, "rep"),
        P("ep", None, "rep"),
        P("ep", "rep", None),
        P("rep", None),
    )
    return jax.shard_map(layer, mesh=mesh, in_specs=in_specs, out_specs=out_specs, check_vma=False)
```

```python
import contextlib
import functools

import jax
import jax.numpy as jnp
from jax import lax
from jax.experimental import pallas as pl
from jax.experimental.pallas import tpu as pltpu
from jax.sharding import PartitionSpec as P


TOP = 2
BF = jnp.bfloat16
F32 = jnp.float32
HI = lax.Precision.HIGHEST
ANY = pl.BlockSpec(memory_space=pl.ANY)


def mm(a, b):
    return jnp.dot(a, b, preferred_element_type=F32)


def mm_nt(a, b, precision=None):
    return lax.dot_general(
        a, b, (((1,), (1,)), ((), ())), preferred_element_type=F32, precision=precision
    )


def mm_tn(a, b, precision=None):
    return lax.dot_general(
        a, b, (((0,), (0,)), ((), ())), preferred_element_type=F32, precision=precision
    )


def call(kernel, grid, scalars, ins, outs, scratch=(), alias=None, flops=0, vmem=20):
    return pallas(kernel, grid, scalars, ins, outs, scratch, alias, flops, vmem)


def pallas(kernel, grid, scalars, ins, outs, scratch, alias, flops, vmem):
    return pl.pallas_call(
        kernel,
        grid_spec=pltpu.PrefetchScalarGridSpec(
            num_scalar_prefetch=len(scalars),
            grid=grid,
            in_specs=[spec for _, spec in ins],
            out_specs=[spec for _, spec in outs],
            scratch_shapes=list(scratch),
        ),
        out_shape=[shape for shape, _ in outs],
        input_output_aliases=alias or {},
        compiler_params=pltpu.CompilerParams(vmem_limit_bytes=vmem << 20),
        cost_estimate=pl.CostEstimate(flops=flops, bytes_accessed=flops // 1000, transcendentals=0),
    )(*scalars, *[array for array, _ in ins])


def whole(array):
    rank = len(array.shape)
    return pl.BlockSpec(array.shape, lambda *_: (0,) * rank)


def shape(dims, kind):
    return jax.ShapeDtypeStruct(dims, kind)


def rows_iota(rows, cols):
    return lax.broadcasted_iota(jnp.int32, (rows, cols), 0)


def slots_of(ids, step, experts, capacity, tok_rows):
    first = ids[TOP * step : TOP * step + 1, :]
    second = ids[TOP * step + 1 : TOP * step + 2, :]
    numbers = rows_iota(max(8, experts), tok_rows)
    hit_first = numbers == first
    hit_second = numbers == second
    named = (hit_first | hit_second).astype(F32)
    earlier = rows_iota(tok_rows, tok_rows) < lax.broadcasted_iota(
        jnp.int32, (tok_rows, tok_rows), 1
    )
    before = mm(named.astype(BF), earlier.astype(F32).astype(BF))
    place_first = jnp.sum(jnp.where(hit_first, before, 0.0), axis=0, keepdims=True)
    place_second = jnp.sum(jnp.where(hit_second, before, 0.0), axis=0, keepdims=True)
    return (
        first * capacity + place_first.astype(jnp.int32),
        second * capacity + place_second.astype(jnp.int32),
    )


def match(slots, step, expert, capacity, tok_rows):
    numbers = rows_iota(capacity, tok_rows) + expert * capacity
    return (
        numbers == slots[TOP * step : TOP * step + 1, :],
        numbers == slots[TOP * step + 1 : TOP * step + 2, :],
    )


def ones_of(mask):
    return mask.astype(F32).astype(BF)


def pack_tokens(me, ids, tokens, router, *outs, micro, experts, capacity):
    packed, partial, slots_out = outs[:-2], outs[-2], outs[-1]
    tok_rows = tokens.shape[1]
    listed = ids[...]
    for step in range(micro):
        first, second = slots_of(listed, step, experts, capacity, tok_rows)
        slots_out[TOP * step : TOP * step + 1, :] = first
        slots_out[TOP * step + 1 : TOP * step + 2, :] = second
        partial[experts * step : experts * (step + 1), :] = mm_nt(router[...], tokens[step])
    slots = slots_out[...]
    for turn in range(experts):
        for step in range(micro):
            a, b = match(slots, step, lax.rem(me[0] + turn, experts), capacity, tok_rows)
            packed[turn][step] = mm(ones_of(a | b), tokens[step]).astype(BF)


def pack_cots(me, ids, slots, logits, cots, *outs, micro, experts, capacity):
    packed, gates = outs[:-1], outs[-1]
    tok_rows = cots.shape[1]
    for step in range(micro):
        chosen = []
        for k in range(TOP):
            row = TOP * step + k
            named = rows_iota(experts, tok_rows) == ids[row : row + 1, :]
            part = logits[experts * step : experts * (step + 1), :]
            chosen.append(jnp.sum(jnp.where(named, part, 0.0), axis=0, keepdims=True))
        spread = chosen[0] - chosen[1]
        gates[TOP * step : TOP * step + 1, :] = jax.nn.sigmoid(spread)
        gates[TOP * step + 1 : TOP * step + 2, :] = jax.nn.sigmoid(-spread)
    listed = slots[...]
    for step in range(micro):
        for turn in range(experts):
            a, b = match(listed, step, lax.rem(me[0] + turn, experts), capacity, tok_rows)
            weight = jnp.where(a, gates[TOP * step : TOP * step + 1, :], 0.0) + jnp.where(
                b, gates[TOP * step + 1 : TOP * step + 2, :], 0.0
            )
            weight = jnp.sum(weight, axis=1, keepdims=True)
            packed[turn][step] = (mm(ones_of(a | b), cots[step]) * weight).astype(BF)


def assemble(rank, pieces, plan, out):
    for piece, entries in zip(pieces, plan):
        slots, width = piece.shape[1:]
        for i, (row, k) in enumerate(entries):
            at = pl.multiple_of(jnp.bitwise_xor(rank, k) * width, 128)
            out[row : row + slots, pl.ds(at, width)] = piece[i]


@contextlib.contextmanager
def keep_rows(rank, pieces, plan, rows, rows_out, sem):
    copy = pltpu.make_async_copy(rows, rows_out, sem)

    @pl.when(pl.program_id(0) == 0)
    def _():
        assemble(rank[0], pieces, plan, rows)
        copy.start()

    yield

    @pl.when(pl.program_id(0) == pl.num_programs(0) - 1)
    def _():
        copy.wait()


def pre_kernel(rank, *refs, plan):
    pieces = refs[: len(plan)]
    gate_w, up_w, rows_out, hidden, pre_gate, pre_up, rows, sem = refs[len(plan) :]

    with keep_rows(rank, pieces, plan, rows, rows_out, sem):
        pre_tile(rows, gate_w, up_w, hidden, pre_gate, pre_up)


def pre_tile(rows, gate_w, up_w, hidden, pre_gate, pre_up):
    gate = mm(rows[...], gate_w[...])
    up = mm(rows[...], up_w[...])
    pre_gate[...] = gate
    pre_up[...] = up
    hidden[...] = (gate * jax.nn.sigmoid(gate) * up).astype(BF)


def grad_kernel(rank, *refs, plan):
    pieces = refs[: len(plan)]
    down_w, hidden, pre_gate, pre_up, _, rows_out, gate_grad, up_grad, dots, rows, acc, sem = refs[
        len(plan) :
    ]
    at = pl.program_id(0)

    @pl.when(at == 0)
    def _():
        acc[...] = jnp.zeros_like(acc)

    with keep_rows(rank, pieces, plan, rows, rows_out, sem):
        grad = mm_nt(rows[...], down_w[...])
        gate = pre_gate[...]
        sig = jax.nn.sigmoid(gate)
        gate_grad[...] = (grad * pre_up[...] * (sig * (1.0 + gate * (1.0 - sig)))).astype(BF)
        up_grad[...] = (grad * (gate * sig)).astype(BF)
        product = grad * hidden[...].astype(F32)
        total = acc[...]
        for i in range(product.shape[1] // 128):
            total = total + product[:, 128 * i : 128 * (i + 1)]
        acc[...] = total

        @pl.when(at == pl.num_programs(0) - 1)
        def _():
            dots[...] = mm_nt(jnp.ones((8, 128), F32), acc[...], HI)


def spread(total, plan, outs):
    slots = outs[0].shape[1]
    for i, places in enumerate(plan):

        @pl.when(pl.program_id(0) == i)
        def _():
            for step, (which, at) in enumerate(places):
                outs[which][at] = total[step * slots : (step + 1) * slots, :]


def out_send_kernel(rank, hidden, down_w, _, out):
    out[...] = mm(hidden[...], down_w[...]).astype(BF)


def out_keep_kernel(rank, hidden, down_w, recv, _, *outs):
    total = (mm(hidden[...], down_w[...]) + recv[...].astype(F32)).astype(BF)
    for i, out in enumerate(outs):
        pl.when(pl.program_id(0) == i)(functools.partial(out.__setitem__, Ellipsis, total))


def in_send_kernel(rank, gate_g, up_g, gate_w, up_w, _, out):
    out[...] = (mm_nt(gate_g[...], gate_w[...]) + mm_nt(up_g[...], up_w[...])).astype(BF)


def in_keep_kernel(rank, gate_g, up_g, gate_w, up_w, recv, _, *outs, plan):
    total = mm_nt(gate_g[...], gate_w[...]) + mm_nt(up_g[...], up_w[...])
    spread((total + recv[...].astype(F32)).astype(BF), plan, outs)


def add_kernel(kept, recv, kept_out, sent_out):
    half = kept_out.shape[0]
    for i in range(2 * half):
        out = kept_out if i < half else sent_out
        out[i % half] = (kept[i].astype(F32) + recv[i].astype(F32)).astype(BF)


def sum_kernel(*refs, micro):
    ins, outs = refs[: 2 * micro], refs[2 * micro :]
    rows = outs[0].shape[1]
    for i, out in enumerate(outs):
        for step in range(micro):
            kept = ins[2 * step][0, i * rows : (i + 1) * rows, :].astype(F32)
            recv = ins[2 * step + 1][0, i * rows : (i + 1) * rows, :].astype(F32)
            out[step] = (kept + recv).astype(BF)


def sum_all_kernel(*refs):
    outs = [ref for ref in refs if len(ref.shape) == 3]
    terms = refs[: len(refs) - len(outs)]
    micro, rows, _ = outs[0].shape
    for step in range(micro):
        for i, out in enumerate(outs):
            at = (step * len(outs) + i) * rows
            total = terms[0][at : at + rows, :].astype(F32)
            for term in terms[1:]:
                total = total + term[at : at + rows, :].astype(F32)
            out[step] = total.astype(BF)


def weight_in_kernel(rows, gate_g, up_g, *refs):
    gate_out, up_out = refs[-2:]
    left = rows[...]
    gate_out[0] = mm_tn(left, gate_g[...]).astype(BF)
    up_out[0] = mm_tn(left, up_g[...]).astype(BF)


def weight_down_kernel(hidden, cots, _, out):
    out[0] = mm_tn(hidden[...], cots[...]).astype(BF)


def column_of(gates, tok_rows):
    eye = (
        rows_iota(tok_rows, tok_rows) == lax.broadcasted_iota(jnp.int32, (tok_rows, tok_rows), 1)
    ).astype(F32)
    return mm_nt(eye, gates, HI)


def mix_kernel(me, slots, gates, *refs, micro, experts, capacity):
    blocks, out = refs[:-1], refs[-1]
    tok_rows = out.shape[1]
    columns = column_of(gates[...], tok_rows)
    listed = slots[...]
    for step in range(micro):
        picked = [0.0] * TOP
        for turn in range(experts):
            hot = match(listed, step, lax.rem(me[0] + turn, experts), capacity, tok_rows)
            block = blocks[turn][step]
            for k in range(TOP):
                picked[k] = picked[k] + mm_tn(ones_of(hot[k]), block)
        total = 0.0
        for k in range(TOP):
            total = total + columns[:, TOP * step + k : TOP * step + k + 1] * picked[k]
        out[step] = total.astype(BF)


def logit_kernel(me, ids, slots, gates, tokens, dots, logit_grad, router, *, micro, experts, capacity):
    tok_rows = tokens.shape[1]
    listed = slots[...]
    total = 0.0
    for step in range(micro):
        scaled = [0.0] * TOP
        for turn in range(experts):
            hot = match(listed, step, lax.rem(me[0] + turn, experts), capacity, tok_rows)
            for k in range(TOP):
                scaled[k] = scaled[k] + lax.dot_general(
                    dots[turn], hot[k].astype(F32), (((1,), (0,)), ((), ())),
                    preferred_element_type=F32, precision=HI,
                )[step : step + 1, :]
        delta = (
            scaled[0] * gates[TOP * step + 1 : TOP * step + 2, :]
            - scaled[1] * gates[TOP * step : TOP * step + 1, :]
        )
        rows = logit_grad.shape[0] // micro
        numbers = rows_iota(rows, tok_rows)
        first = numbers == ids[TOP * step : TOP * step + 1, :]
        second = numbers == ids[TOP * step + 1 : TOP * step + 2, :]
        grad = jnp.where(first, delta, 0.0) - jnp.where(second, delta, 0.0)
        logit_grad[step * rows : (step + 1) * rows, :] = grad
        total = total + lax.dot_general(
            grad, tokens[step].astype(F32), (((1,), (0,)), ((), ())),
            preferred_element_type=F32, precision=HI,
        )
    router[...] = total


def unpack_kernel(me, slots, logit_grad, router, *refs, micro, experts, capacity):
    blocks, out = refs[:-1], refs[-1]
    tok_rows = out.shape[1]
    listed = slots[...]
    rows = logit_grad.shape[0] // micro
    for step in range(micro):
        total = mm_tn(
            logit_grad[step * rows : step * rows + experts, :], router[...].astype(F32), HI
        )
        for turn in range(experts):
            a, b = match(listed, step, lax.rem(me[0] + turn, experts), capacity, tok_rows)
            total = total + mm_tn(ones_of(a | b), blocks[turn][step])
        out[step] = total.astype(BF)


def layer(tokens, expert_ids, router_weight, w_gate, w_up, w_down, cotangent):
    micro, tok_rows, width = tokens.shape
    experts = router_weight.shape[1]
    ranks = lax.axis_size("rep")
    places = lax.axis_size("ep")
    assert places == experts and ranks & (ranks - 1) == 0 and ranks > 2
    half = ranks // 2
    capacity = min(tok_rows, 3 * tok_rows * TOP // (2 * experts))
    slots_n = places * capacity
    gate_w, up_w, down_w = w_gate[0], w_up[0], w_down[0]
    features, units = gate_w.shape
    rank = lax.axis_index("rep").reshape(1)
    me = lax.axis_index("ep").reshape(1)
    sizes = dict(micro=micro, experts=experts, capacity=capacity)

    def swap(value, bits):
        return lax.ppermute(value, "rep", [(i, i ^ bits) for i in range(ranks)])

    def shift(value, turn):
        return lax.ppermute(value, "ep", [(i, (i + turn) % places) for i in range(places)])

    def far(array):
        return pltpu.with_memory_space_constraint(array, pltpu.HBM)

    def full(array):
        return (array, whole(array))

    ids = jnp.transpose(expert_ids, (0, 2, 1)).reshape(micro * TOP, tok_rows)
    router = router_weight.T

    block = shape((micro, capacity, width), BF)
    token_rows = shape((micro * TOP, tok_rows), jnp.int32)
    logit_rows = shape((micro * experts, tok_rows), F32)
    *packed, logits, slots = call(
        functools.partial(pack_tokens, **sizes), (1,), [me],
        [full(far(ids)), full(far(tokens)), full(far(router))],
        [full(block)] * experts + [full(logit_rows), full(token_rows)],
        flops=10**8,
    )
    bits = 1
    while bits < ranks:
        logits = logits + swap(logits, bits)
        bits *= 2
    *cots, gates = call(
        functools.partial(pack_cots, **sizes), (1,), [me],
        [full(ids), full(slots), full(logits), full(cotangent)],
        [full(block)] * experts + [full(shape((micro * TOP, tok_rows), F32))],
        flops=10**8,
    )
    chip_bits = [1 << i for i in range(1, ranks.bit_length() - 1)]
    order = [chip_bits[m % len(chip_bits) :] + chip_bits[: m % len(chip_bits)] for m in range(micro)]

    def dispatch(blocks):
        got = [blocks[0]]
        for turn in range(1, places):
            got.append(shift(blocks[turn], turn))
        return got

    def to_partner(pieces, plan):
        for i in range(len(pieces)):
            pieces.append(swap(pieces[i], 1))
            plan.append([(row, k ^ 1) for row, k in plan[i]])
        return pieces, plan

    def gather_by_steps(blocks):
        got = dispatch(blocks)
        pieces, plan = [], []
        for parts, base in ((got[:1], 0), (got[1:], capacity)):
            held, numbers = [], []
            for step in range(micro):
                held.append(jnp.concatenate([part[step : step + 1] for part in parts], axis=1))
                numbers.append([(step * slots_n + base, 0)])
            for stage in range(len(chip_bits)):
                for step in range(micro):
                    bit = order[step][stage]
                    recv = swap(held[step], bit)
                    there = [(row, k ^ bit) for row, k in numbers[step]]
                    if stage == len(chip_bits) - 1:
                        pieces += [held[step], recv]
                        plan += [numbers[step], there]
                    else:
                        held[step] = jnp.concatenate([held[step], recv], axis=0)
                        numbers[step] = numbers[step] + there
        return to_partner(pieces, plan)

    def gather_at_once(blocks):
        own = jnp.concatenate(dispatch(blocks), axis=1)
        pieces = [own] + [swap(own, 2 * k) for k in range(1, half)]
        plan = [[(step * slots_n, 2 * k) for step in range(micro)] for k in range(half)]
        return to_partner(pieces, plan)

    token_pieces, token_plan = gather_by_steps(packed)
    cot_pieces, cot_plan = gather_at_once(cots)

    tile = min(256, units)
    steps = units // tile
    all_rows = micro * slots_n
    work = 2 * all_rows * features * units
    columns = pl.BlockSpec((all_rows, tile), lambda i, *_: (0, i))
    rows_shape = shape((all_rows, features), BF)
    units_shape = shape((all_rows, units), BF)
    wide_shape = shape((all_rows, units), F32)

    weight = pl.BlockSpec((features, tile), lambda i, *_: (0, i))
    rows_in, hidden, pre_gate, pre_up = call(
        functools.partial(pre_kernel, plan=token_plan), (steps,), [rank],
        [full(p) for p in token_pieces] + [(far(gate_w), weight), (far(up_w), weight)],
        [(rows_shape, ANY), (units_shape, columns)] + [(wide_shape, columns)] * 2,
        scratch=[pltpu.VMEM((all_rows, features), BF), pltpu.SemaphoreType.DMA],
        flops=2 * work,
        vmem=36,
    )
    sent = shape((half, all_rows, width), BF)
    kept = shape((half // 2, slots_n, width), BF)
    by_step = pl.BlockSpec((None, all_rows, width), lambda i, *_: (i, 0, 0))
    lists = []
    for step in range(micro):
        numbers = [0]
        for bit in order[step]:
            numbers = numbers + [k ^ bit for k in numbers]
        lists.append(numbers)
    homes = []
    for i in range(half):
        at = [lists[step].index(2 * i) for step in range(micro)]
        homes.append(
            [(2 * step + at[step] // (half // 2), at[step] % (half // 2)) for step in range(micro)]
        )

    def wide(odd):
        return pl.BlockSpec((units, width), lambda i, r: (0, jnp.bitwise_xor(r[0], 2 * i + odd)))

    def tall(odd):
        return pl.BlockSpec((width, units), lambda i, r: (jnp.bitwise_xor(r[0], 2 * i + odd), 0))

    def reduce(parts):
        parts = list(parts)
        for stage in reversed(range(len(chip_bits))):
            for step in range(micro):
                mine, theirs = parts[2 * step], parts[2 * step + 1]
                recv = swap(theirs, order[step][stage])
                if stage == 0:
                    parts[2 * step + 1] = recv
                else:
                    smaller = shape((mine.shape[0] // 2,) + mine.shape[1:], BF)
                    parts[2 * step], parts[2 * step + 1] = call(
                        add_kernel, (1,), [], [full(mine), full(recv)], [full(smaller)] * 2, flops=10**7
                    )
        blocks = call(
            functools.partial(sum_kernel, micro=micro), (1,), [],
            [full(part) for part in parts], [full(block)] * places, flops=10**7,
        )
        return send_home(blocks)

    def send_home(blocks):
        return [blocks[0]] + [shift(blocks[turn], -turn) for turn in range(1, places)]

    (out_sent,) = call(
        out_send_kernel, (half,), [rank],
        [full(hidden), (far(down_w), wide(1)), (hidden, ANY)], [(sent, by_step)], flops=work // 2,
    )
    out_parts = call(
        out_keep_kernel, (half,), [rank],
        [full(hidden), (far(down_w), wide(0)), (swap(out_sent, 1), by_step), (hidden, ANY)],
        [full(shape((all_rows, width), BF))] * half, flops=work // 2,
    )
    out_terms = [out_parts[0]] + [swap(out_parts[k], 2 * k) for k in range(1, half)]
    out_blocks = send_home(
        call(sum_all_kernel, (1,), [], [full(t) for t in out_terms], [full(block)] * places, flops=10**7)
    )

    weight = pl.BlockSpec((tile, features), lambda i, *_: (i, 0))
    rows_cot, gate_g, up_g, dots = call(
        functools.partial(grad_kernel, plan=cot_plan), (steps,), [rank],
        [full(p) for p in cot_pieces]
        + [(far(down_w), weight), (hidden, columns), (pre_gate, columns), (pre_up, columns)]
        + [(out_parts[0], ANY)],
        [(rows_shape, ANY), (units_shape, columns), (units_shape, columns)]
        + [full(shape((8, all_rows), F32))],
        scratch=[pltpu.VMEM((all_rows, features), BF), pltpu.VMEM((all_rows, 128), F32), pltpu.SemaphoreType.DMA],
        flops=work,
        vmem=36,
    )
    (in_sent,) = call(
        in_send_kernel, (half,), [rank],
        [full(gate_g), full(up_g), (far(gate_w), tall(1)), (far(up_w), tall(1)), (dots, ANY)],
        [(sent, by_step)], flops=work,
    )
    in_parts = call(
        functools.partial(in_keep_kernel, plan=homes), (half,), [rank],
        [full(gate_g), full(up_g), (far(gate_w), tall(0)), (far(up_w), tall(0))]
        + [(swap(in_sent, 1), by_step), (in_sent, ANY)],
        [full(kept)] * (2 * micro), flops=work, vmem=26,
    )
    in_blocks = reduce(in_parts)
    span = min(512, features)
    rows_span = pl.BlockSpec((all_rows, span), lambda i: (0, i))
    part = features // span // 2
    grads = [in_parts[0]]
    for base in (0, part):
        weight_spec = pl.BlockSpec((1, span, units), lambda i, base=base: (0, i + base, 0))
        rows_part = pl.BlockSpec((all_rows, span), lambda i, base=base: (0, i + base))
        grads = call(
            weight_in_kernel, (part,), [],
            [(far(rows_in), rows_part), full(gate_g), full(up_g)] + [(far(g) if base else g, ANY) for g in grads],
            [(pltpu.HBM((1, features, units), BF), weight_spec)] * 2,
            alias={3: 0, 4: 1} if base else None,
            flops=work,
        )
    gate_grad, up_grad = grads
    span = min(1024, features)
    rows_span = pl.BlockSpec((all_rows, span), lambda i: (0, i))
    down_spec = pl.BlockSpec((1, units, span), lambda i: (0, 0, i))
    (down_grad,) = call(
        weight_down_kernel, (features // span,), [],
        [full(hidden), (far(rows_cot), rows_span), (dots, ANY)],
        [(pltpu.HBM((1, units, features), BF), down_spec)],
        flops=work,
    )

    scaled = dots[0].reshape(micro, places, capacity)
    scaled = jnp.pad(scaled, ((0, 8 - micro), (0, 0), (0, 0)))
    home = jnp.stack([scaled[:, 0]] + [shift(scaled[:, turn], -turn) for turn in range(1, places)])
    bits = 1
    while bits < ranks:
        home = home + swap(home, bits)
        bits *= 2
    (mixed,) = call(
        functools.partial(mix_kernel, **sizes), (1,), [me],
        [full(slots), full(gates)] + [full(b) for b in out_blocks],
        [full(shape(tokens.shape, BF))], flops=10**8,
    )
    padded = max(8, experts)
    logit_grad, router_grad = call(
        functools.partial(logit_kernel, **sizes), (1,), [me],
        [full(ids), full(slots), full(gates), full(tokens), full(home)],
        [full(shape((micro * padded, tok_rows), F32)), full(shape((padded, width), F32))],
        flops=10**8,
    )
    bits = 1
    while bits < places:
        theirs = lax.ppermute(router_grad, "ep", [(i, i ^ bits) for i in range(places)])
        router_grad = router_grad + theirs
        bits *= 2
    (token_grad,) = call(
        functools.partial(unpack_kernel, **sizes), (1,), [me],
        [full(slots), full(logit_grad), full(router)] + [full(b) for b in in_blocks],
        [full(shape(tokens.shape, BF))], flops=10**8,
    )
    return mixed, token_grad, gate_grad, up_grad, down_grad, router_grad[:experts].T


def solution(mesh):
    in_specs = (
        P(None, "ep", "rep"),
        P(None, "ep", None),
        P("rep", None),
        P("ep", None, "rep"),
        P("ep", None, "rep"),
        P("ep", "rep", None),
        P(None, "ep", "rep"),
    )
    out_specs = (
        P(None, "ep", "rep"),
        P(None, "ep", "rep"),
        P("ep", None, "rep"),
        P("ep", None, "rep"),
        P("ep", "rep", None),
        P("rep", None),
    )
    return jax.shard_map(layer, mesh=mesh, in_specs=in_specs, out_specs=out_specs, check_vma=False)
```
